32 devices in a mesh: dp: 4 (over y, core), vocab: 8 (over z, x).
Axes of the slice: x: 2, y: 2, z: 4, core: 2. Of those that a mesh axis runs over, the one named last changes fastest.
Arguments:
- teacher_hidden: bfloat16 [512, 16384], P('dp', 'vocab'), may hold values from -120 to 120
- student_hidden: bfloat16 [512, 4096], P('dp', 'vocab'), may hold values from -120 to 120
- teacher_weight: bfloat16 [16384, 65536], P('dp', 'vocab'), may hold values from -1 to 1
- student_weight: bfloat16 [4096, 65536], P('dp', 'vocab'), may hold values from -1 to 1
Outputs:
- kl: float32 [512], P('dp')
- loss: float32 [], replicated
The draws below stay inside these ranges and needn't reach their ends.
All inputs are finite; a program needn't handle non-finite values.
Results may differ from the reference program's by a relative error of at most 0.0003.
Values may be sent and summed in bfloat16 or wider, within the bound.
A program may use at most 256 MiB of HBM per device.

```python
import jax
import jax.numpy as jnp

HT = 16384
HS = 4096
V = 65536
TOKENS = 512


def weight_block(key, offset, features, block_id):
    normals = jax.random.normal(jax.random.fold_in(jax.random.fold_in(key, offset), block_id), (features, 128), jnp.float32)
    return jnp.clip(normals, -6.0, 6.0) * features ** (-0.5)


def teacher_block(key, block_id):
    return weight_block(key, 101, HT, block_id)


def student_block(key, block_id):
    folded = teacher_block(key, block_id).reshape(HT // HS, HS, 128).sum(axis=0)
    own_noise = weight_block(key, 202, HS, block_id)
    return jnp.clip(folded + 0.1 * own_noise, -1.0, 1.0)


def stack_blocks(key, block_fn, features):
    tile_stack = jax.vmap(lambda block_id: block_fn(key, block_id))(jnp.arange(V // 128))
    return jnp.transpose(tile_stack, (1, 0, 2)).reshape(features, V)


def shared_rows(key):
    common = jax.random.normal(jax.random.fold_in(key, 11), (TOKENS, HS), jnp.float32) * 3.0
    rising = 1.0 + 0.85 * jnp.arange(TOKENS, dtype=jnp.float32) / TOKENS
    return (common, rising)


def draw_teacher_weight(key, part):
    return stack_blocks(key, teacher_block, HT).astype(jnp.bfloat16)


def draw_student_weight(key, part):
    return stack_blocks(key, student_block, HS).astype(jnp.bfloat16)


def draw_teacher_hidden(key, part):
    common, rising = shared_rows(key)
    own_noise = jax.random.normal(jax.random.fold_in(key, 12), (TOKENS, HT), jnp.float32) * 0.5 * rising[:, None]
    values = jnp.tile(common, (1, HT // HS)) + own_noise
    return jnp.clip(values, -120.0, 120.0).astype(jnp.bfloat16)


def draw_student_hidden(key, part):
    common, rising = shared_rows(key)
    own_noise = jax.random.normal(jax.random.fold_in(key, 32), (TOKENS, HS), jnp.float32) * 0.5 * rising[:, None]
    values = common + own_noise
    return jnp.clip(values, -120.0, 120.0).astype(jnp.bfloat16)


def setup_inputs(seed: int = 0) -> dict:
    keys = jax.random.split(jax.random.key(seed), 5)
    teacher_hidden = draw_teacher_hidden(jax.random.fold_in(keys[4], 71), 0)
    student_hidden = draw_student_hidden(jax.random.fold_in(keys[4], 71), 0)
    teacher_weight = draw_teacher_weight(jax.random.fold_in(keys[4], 71), 0)
    student_weight = draw_student_weight(jax.random.fold_in(keys[4], 71), 0)
    return dict(teacher_hidden=teacher_hidden, student_hidden=student_hidden, teacher_weight=teacher_weight, student_weight=student_weight)


def reference(teacher_hidden, student_hidden, teacher_weight, student_weight):
    teacher_logits = jnp.dot(teacher_hidden, teacher_weight, preferred_element_type=jnp.float32)
    student_logits = jnp.dot(student_hidden, student_weight, preferred_element_type=jnp.float32)
    teacher_top = jnp.max(teacher_logits, axis=1)
    student_top = jnp.max(student_logits, axis=1)
    teacher_exp = jnp.exp(teacher_logits - teacher_top[:, None])
    teacher_total = jnp.sum(teacher_exp, axis=1)
    weighted = jnp.sum(teacher_exp * (teacher_logits - student_logits), axis=1)
    student_total = jnp.sum(jnp.exp(student_logits - student_top[:, None]), axis=1)
    teacher_lse = teacher_top + jnp.log(teacher_total)
    student_lse = student_top + jnp.log(student_total)
    kl = weighted / teacher_total - teacher_lse + student_lse
    loss = jnp.mean(kl)
    return (kl, loss)
```

```python
import functools

import jax
import jax.numpy as jnp
from jax import lax
from jax.experimental import pallas as pl
from jax.experimental.pallas import tpu as pltpu
from jax.sharding import PartitionSpec as P

MESH = pl.DeviceIdType.MESH
SPAN = 240.0
LANES = 128
SLOTS = 3
HOP = 3
SPACE = 4


def encode(block):
    mag = jnp.abs(block)
    top = jnp.max(mag, axis=1, keepdims=True)
    step = jnp.where(top > 0, SPAN / jnp.where(top > 0, top, 1.0), 0.0)
    power = jnp.exp2(mag * step - 0.5 * SPAN)
    return jnp.where(block < 0, -power, power).astype(jnp.bfloat16), top


def decode(code, scale):
    value = code.astype(jnp.float32)
    mag = (jnp.log2(jnp.abs(value)) + 0.5 * SPAN) * scale
    return jnp.where(value < 0, -mag, mag)


def kernel(
    n_dp, n_vocab, cols,
    th_ref, sh_ref, tw_ref, sw_ref, kl_ref, loss_ref,
    hid_t, hid_s, wt, ws, part, pair_a, pair_b, code_out, code_in, top_out, top_in, run,
    st_out, st_in, ls_out, ls_in,
    g_recv, g_send, src_send, w_sem, d_send, d_recv, y_send, y_recv, st_send, st_recv, ls_send, ls_recv,
):
    tok, wide = th_ref.shape
    narrow = sh_ref.shape[1]
    half = tok // 2
    n_y = n_dp // 2
    per = n_vocab // n_dp
    n = tw_ref.shape[1] // cols
    passes = 2 * (n_y - 1)
    n_a = passes * n
    total = n_a + n
    n_slots = 4 * n_y

    d, v = lax.axis_index("dp"), lax.axis_index("vocab")
    y, core = d // 2, lax.rem(d, 2)
    row, col = v // per, lax.rem(v, per)

    def remote(src, dst, send, recv, dp, vocab):
        return pltpu.make_async_remote_copy(
            src_ref=src, dst_ref=dst, send_sem=send, recv_sem=recv,
            device_id={"dp": dp, "vocab": vocab}, device_id_type=MESH,
        )

    def weight_copies(g):
        at = pl.ds(pl.multiple_of(lax.rem(g, n) * cols, LANES), cols)
        slot = lax.rem(g, SLOTS)
        return (
            pltpu.make_async_copy(tw_ref.at[:, at], wt.at[slot], w_sem.at[slot, 0]),
            pltpu.make_async_copy(sw_ref.at[:, at], ws.at[slot], w_sem.at[slot, 1]),
        )

    def weights_start(g):
        for copy in weight_copies(g):
            copy.start()

    for g in range(SLOTS - 1):
        weights_start(jnp.int32(g))

    barrier = pltpu.get_barrier_semaphore()
    for o in range(1, n_dp):
        pl.semaphore_signal(barrier, inc=1, device_id={"dp": lax.rem(d + o, n_dp), "vocab": v}, device_id_type=MESH)
    for o in range(1, n_vocab):
        pl.semaphore_signal(barrier, inc=1, device_id={"dp": d, "vocab": lax.rem(v + o, n_vocab)}, device_id_type=MESH)
    pl.semaphore_wait(barrier, n_dp + n_vocab - 2)

    heads = ((th_ref, hid_t, wide), (sh_ref, hid_s, narrow))

    def region(hid, s, q, width):
        first = s * half
        if not isinstance(first, int):
            first = pl.multiple_of(first, half)
        return hid.at[pl.ds(first, half), pl.ds(pl.multiple_of(q * width, LANES), width)]

    y_to, core_to = row // 2, lax.rem(row, 2)
    k_of, rel = lax.rem(y - y_to + n_y, n_y), lax.rem(core + core_to, 2)
    local = row == d

    def source_copies(k, h):
        s = (k - 1) * 4 + h * 2 + rel if k else (n_y - 1) * 4 + rel * 2 + h
        return [
            remote(
                src.at[pl.ds(h * half, half), :], region(hid, s, col, width),
                src_send.at[h, e], g_recv.at[col, s, e], row, v,
            )
            for e, (src, hid, width) in enumerate(heads)
        ]

    def own_copies(h):
        s = (n_y - 1) * 4 + h
        return [
            pltpu.make_async_copy(
                src.at[pl.ds(h * half, half), :], region(hid, s, col, width), g_recv.at[col, s, e]
            )
            for e, (src, hid, width) in enumerate(heads)
        ]

    for k in range(n_y):

        @pl.when((k_of == k) & jnp.logical_not(local))
        def _(k=k):
            for h in range(2):
                for copy in source_copies(k, h):
                    copy.start()

    @pl.when(local)
    def _():
        for h in range(2):
            for copy in own_copies(h):
                copy.start()

    def arrived(s, q):
        for e, (_, hid, width) in enumerate(heads):
            at = region(hid, s, q, width)
            pltpu.make_async_copy(at, at, g_recv.at[q, s, e]).wait()

    up, down = (row >= d) & (row + 1 < n_dp), (row <= d) & (row > 0)

    def forwards(s, e):
        _, hid, width = heads[e]
        at = region(hid, s, col, width)
        recv = g_recv.at[col, s, e]
        peers = [
            remote(at, at, g_send.at[s, e, 1 + o], recv, d, row * per + lax.rem(col + o, per)) for o in range(1, per)
        ]
        return (
            remote(at, at, g_send.at[s, e, 0], recv, d, lax.rem(v + per, n_vocab)),
            remote(at, at, g_send.at[s, e, 1], recv, d, lax.rem(v + n_vocab - per, n_vocab)),
            peers,
        )

    def relay(s):
        for e, (_, hid, width) in enumerate(heads):
            at = region(hid, s, col, width)
            pltpu.make_async_copy(at, at, g_recv.at[col, s, e]).wait()
            above, below, peers = forwards(s, e)

            @pl.when(up)
            def _():
                above.start()

            @pl.when(down)
            def _():
                below.start()

            for copy in peers:
                copy.start()

    def peers_arrived(s):
        for o in range(1, per):
            arrived(s, lax.rem(col + o, per))

    away = jnp.abs(row - d)

    def matmul(g, first, rows):
        slot, at = lax.rem(g, SLOTS), lax.rem(g, 2)
        where = pl.ds(first, rows)
        part[at, 0, pl.ds(0, rows), :] = jnp.dot(hid_t[where, :], wt[slot], preferred_element_type=jnp.float32)
        part[at, 1, pl.ds(0, rows), :] = jnp.dot(hid_s[where, :], ws[slot], preferred_element_type=jnp.float32)

    partner = d + 1 - 2 * core

    def pair_copy_a(g):
        at = lax.rem(g, 2)
        return remote(
            part.at[at, :, pl.ds(half, half), :], pair_a.at[g], d_send.at[at], d_recv.at[g], partner, v
        )

    def pair_copy_b(i):
        at = lax.rem(n_a + i, 2)
        return remote(
            part.at[at, :, pl.ds(tok, tok), :], pair_b.at[i], d_send.at[at], d_recv.at[n_a + i], partner, v
        )

    def code_copies(g):
        k = g // (2 * n) + 1
        to = lax.rem(y + k, n_y) * 2 + core
        return (
            remote(code_out.at[g], code_in.at[g], y_send.at[g, 0], y_recv.at[g, 0], to, v),
            remote(top_out.at[g], top_in.at[g], y_send.at[g, 1], y_recv.at[g, 1], to, v),
        )

    def code_start(g):
        for copy in code_copies(g):
            copy.start()

    def finish_a(g):
        at = lax.rem(g, 2)
        pair_copy_a(g).wait()
        tops = []
        for e in range(2):
            code, top = encode(part[at, e, pl.ds(0, half), :] + pair_a[g, e])
            code_out[g, e] = code
            tops.append(top)
        tops = jnp.broadcast_to(jnp.concatenate(tops, axis=0), (tok, LANES))
        top_out[g] = tops.T[:8]

    def finish_b(i):
        at = lax.rem(n_a + i, 2)
        pair_copy_b(i).wait()
        for p in range(passes):
            for copy in code_copies(p * n + i):
                copy.wait_recv()
        for h in range(2):
            rows = pl.ds(h * half, half)
            t, s = (part[at, e, rows, :] + pair_b[i, e, rows, :] for e in range(2))
            for k in range(1, n_y):
                g = ((k - 1) * 2 + h) * n + i
                scale = (jnp.broadcast_to(top_in[g][:1], (LANES, tok)).T) * (1.0 / SPAN)
                blocks = cols // LANES
                t = t + decode(code_in[g, 0], jnp.concatenate([scale[:half]] * blocks, axis=1))
                s = s + decode(code_in[g, 1], jnp.concatenate([scale[half:]] * blocks, axis=1))
            ts = [t[:, b * LANES : (b + 1) * LANES] for b in range(cols // LANES)]
            ss = [s[:, b * LANES : (b + 1) * LANES] for b in range(cols // LANES)]
            t_old, s_old = run[0, rows, :], run[1, rows, :]
            t_top = functools.reduce(jnp.maximum, ts, t_old)
            s_top = functools.reduce(jnp.maximum, ss, s_old)
            t_fix = jnp.exp(t_old - t_top)
            t_sum, w_sum = run[2, rows, :] * t_fix, run[3, rows, :] * t_fix
            s_sum = run[4, rows, :] * jnp.exp(s_old - s_top)
            for tb, sb in zip(ts, ss):
                e = jnp.exp(tb - t_top)
                t_sum = t_sum + e
                w_sum = w_sum + e * (tb - sb)
                s_sum = s_sum + jnp.exp(sb - s_top)
            run[0, rows, :], run[1, rows, :] = t_top, s_top
            run[2, rows, :], run[3, rows, :], run[4, rows, :] = t_sum, w_sum, s_sum

    run[pl.ds(0, 2)] = jnp.full((2, tok, LANES), -jnp.inf, jnp.float32)
    run[pl.ds(2, 3)] = jnp.zeros((3, tok, LANES), jnp.float32)

    for s in range(2):
        relay(s)

    def step_a(g, _):
        @pl.when(g >= 1)
        def _():
            pair_copy_a(g - 1).start()

        @pl.when(g >= 2)
        def _():
            code_start(g - 2)

        for s in range(2, n_slots):
            deadline = min(s // 2, passes) * n - 1
            usual = 1 + SPACE * (s - 2) + HOP * away

            @pl.when(g == jnp.minimum(usual, deadline))
            def _(s=s):
                relay(s)

        p = g // n

        @pl.when(lax.rem(g, n) == 0)
        def _():
            for q in range(passes):

                @pl.when(p == q)
                def _(q=q):
                    peers_arrived(2 * q)
                    peers_arrived(2 * q + 1)

        for copy in weight_copies(g):
            copy.wait()
        weights_start(g + SLOTS - 1)
        matmul(g, pl.multiple_of(p * tok, tok), tok)

        @pl.when(g >= 1)
        def _():
            finish_a(g - 1)

        return 0

    lax.fori_loop(0, n_a, step_a, 0)

    pair_copy_a(jnp.int32(n_a - 1)).start()
    code_start(jnp.int32(n_a - 2))
    for s in range(4 * (n_y - 1), n_slots):
        peers_arrived(s)

    def step_b(i, _):
        g = n_a + i

        @pl.when(i >= 1)
        def _():
            pair_copy_b(i - 1).start()

        @pl.when(i == 1)
        def _():
            code_start(jnp.int32(n_a - 1))

        for copy in weight_copies(g):
            copy.wait()

        @pl.when(g + SLOTS - 1 < total)
        def _():
            weights_start(g + SLOTS - 1)

        matmul(g, passes * tok, 2 * tok)

        @pl.when(i == 0)
        def _():
            finish_a(jnp.int32(n_a - 1))

        @pl.when(i >= 1)
        def _():
            finish_b(i - 1)

        return 0

    lax.fori_loop(0, n, step_b, 0)
    pair_copy_b(jnp.int32(n - 1)).start()
    finish_b(jnp.int32(n - 1))

    t_lane, s_lane = run[0], run[1]
    t_top = jnp.max(t_lane, axis=1, keepdims=True)
    s_top = jnp.max(s_lane, axis=1, keepdims=True)
    t_fix = jnp.exp(t_lane - t_top)
    t_sum = jnp.sum(run[2] * t_fix, axis=1, keepdims=True)
    w_sum = jnp.sum(run[3] * t_fix, axis=1, keepdims=True)
    s_sum = jnp.sum(run[4] * jnp.exp(s_lane - s_top), axis=1, keepdims=True)
    lane = lax.broadcasted_iota(jnp.int32, (tok, LANES), 1)
    table = jnp.zeros((tok, LANES), jnp.float32)
    for i, stat in enumerate((t_top, s_top, t_sum, w_sum, s_sum)):
        table = jnp.where(lane == i, stat, table)
    table = table.T[:8]
    st_out[...] = table
    st_in[v] = table

    for k in range(n_y):

        @pl.when((k_of == k) & jnp.logical_not(local))
        def _(k=k):
            for h in range(2):
                for copy in source_copies(k, h):
                    copy.wait_send()

    def drain_codes(g, _):
        for copy in code_copies(g):
            copy.wait_send()
        return 0

    lax.fori_loop(0, n_a, drain_codes, 0)

    for s in range(n_slots):
        for e in range(2):
            above, below, peers = forwards(s, e)

            @pl.when(up)
            def _():
                above.wait_send()

            @pl.when(down)
            def _():
                below.wait_send()

            for copy in peers:
                copy.wait_send()

    def stat_copy(to, holder):
        return remote(st_out, st_in.at[holder], st_send.at[to], st_recv.at[holder], d, to)

    others = [lax.rem(v + o, n_vocab) for o in range(1, n_vocab)]
    for o in others:
        stat_copy(o, v).start()
    for o in others:
        stat_copy(v, o).wait_recv()

    def field(holder, i):
        return st_in[holder, pl.ds(i, 1), :]

    t_max = functools.reduce(jnp.maximum, [field(q, 0) for q in range(n_vocab)])
    s_max = functools.reduce(jnp.maximum, [field(q, 1) for q in range(n_vocab)])
    t_total = weighted = s_total = jnp.zeros((1, tok), jnp.float32)
    for q in range(n_vocab):
        scale = jnp.exp(field(q, 0) - t_max)
        t_total = t_total + scale * field(q, 2)
        weighted = weighted + scale * field(q, 3)
        s_total = s_total + jnp.exp(field(q, 1) - s_max) * field(q, 4)
    kl = weighted / t_total - (t_max + jnp.log(t_total)) + (s_max + jnp.log(s_total))
    kl_ref[...] = kl
    mine = jnp.broadcast_to(jnp.sum(kl, axis=1, keepdims=True), (8, LANES))
    ls_out[...] = mine
    ls_in[d] = mine
    for o in others:
        stat_copy(o, v).wait_send()

    def loss_copy(to, holder):
        return remote(ls_out, ls_in.at[holder], ls_send.at[to], ls_recv.at[holder], to, v)

    others = [lax.rem(d + o, n_dp) for o in range(1, n_dp)]
    for o in others:
        loss_copy(o, d).start()
    for o in others:
        loss_copy(d, o).wait_recv()
    loss = functools.reduce(jnp.add, [ls_in[q] for q in range(n_dp)]) / (tok * n_dp)
    loss_ref[...] = loss[:1, :1]
    for o in others:
        loss_copy(o, d).wait_send()


def shards(teacher_hidden, student_hidden, teacher_weight, student_weight):
    n_dp, n_vocab = lax.axis_size("dp"), lax.axis_size("vocab")
    tok, wide = teacher_hidden.shape
    narrow = student_hidden.shape[1]
    deep, local_cols = teacher_weight.shape
    shallow = student_weight.shape[0]
    cols = min(512, local_cols)
    n, n_y, per, half = local_cols // cols, n_dp // 2, n_vocab // n_dp, tok // 2
    n_a = 2 * (n_y - 1) * n
    slots = 4 * n_y
    bf16, f32, dma = jnp.bfloat16, jnp.float32, pltpu.SemaphoreType.DMA
    hbm = pl.BlockSpec(memory_space=pl.ANY)
    vmem = pl.BlockSpec(memory_space=pltpu.VMEM)
    kl, loss = pl.pallas_call(
        functools.partial(kernel, n_dp, n_vocab, cols),
        out_shape=(jax.ShapeDtypeStruct((1, tok), f32), jax.ShapeDtypeStruct((1, 1), f32)),
        in_specs=[hbm] * 4,
        out_specs=(vmem, vmem),
        scratch_shapes=[
            pltpu.VMEM((n_dp * tok, deep), bf16),
            pltpu.VMEM((n_dp * tok, shallow), bf16),
            pltpu.VMEM((SLOTS, deep, cols), bf16),
            pltpu.VMEM((SLOTS, shallow, cols), bf16),
            pltpu.VMEM((2, 2, 2 * tok, cols), f32),
            pltpu.VMEM((n_a, 2, half, cols), f32),
            pltpu.VMEM((n, 2, tok, cols), f32),
            pltpu.VMEM((n_a, 2, half, cols), bf16),
            pltpu.VMEM((n_a, 2, half, cols), bf16),
            pltpu.VMEM((n_a, 8, tok), f32),
            pltpu.VMEM((n_a, 8, tok), f32),
            pltpu.VMEM((5, tok, LANES), f32),
            pltpu.VMEM((8, tok), f32),
            pltpu.VMEM((n_vocab, 8, tok), f32),
            pltpu.VMEM((8, LANES), f32),
            pltpu.VMEM((n_dp, 8, LANES), f32),
            dma((per, slots, 2)),
            dma((slots, 2, per + 1)),
            dma((2, 2)),
            dma((SLOTS, 2)),
            dma((2,)),
            dma((n_a + n,)),
            dma((n_a, 2)),
            dma((n_a, 2)),
            dma((n_vocab,)),
            dma((n_vocab,)),
            dma((n_dp,)),
            dma((n_dp,)),
        ],
        compiler_params=pltpu.CompilerParams(
            collective_id=0, has_side_effects=True, vmem_limit_bytes=64 * 1024 * 1024 - 65536
        ),
    )(teacher_hidden, student_hidden, teacher_weight, student_weight)
    return kl.reshape(tok), loss.reshape(())


def solution(mesh):
    in_specs = (P("dp", "vocab"), P("dp", "vocab"), P("dp", "vocab"), P("dp", "vocab"))
    out_specs = (P("dp"), P())
    return jax.shard_map(shards, mesh=mesh, in_specs=in_specs, out_specs=out_specs, check_vma=False)
```

```python
import functools

import jax
import jax.numpy as jnp
from jax import lax
from jax.experimental import pallas as pl
from jax.experimental.pallas import tpu as pltpu
from jax.sharding import PartitionSpec as P

MESH = pl.DeviceIdType.MESH
SPAN = 240.0
LANES = 128
SLOTS = 3
HOP = 2
SPACE = 4
LATE = 14


def encode(block):
    mag = jnp.abs(block)
    top = jnp.max(mag, axis=1, keepdims=True)
    step = jnp.where(top > 0, SPAN / jnp.where(top > 0, top, 1.0), 0.0)
    power = jnp.exp2(mag * step - 0.5 * SPAN)
    return jnp.where(block < 0, -power, power).astype(jnp.bfloat16), top


def decode(code, scale):
    value = code.astype(jnp.float32)
    mag = (jnp.log2(jnp.abs(value)) + 0.5 * SPAN) * scale
    return jnp.where(value < 0, -mag, mag)


def kernel(
    n_dp, n_vocab, cols,
    th_ref, sh_ref, tw_ref, sw_ref, kl_ref, loss_ref,
    hid_t, hid_s, wt, ws, part, pair_q, pair_r, pair_b, out_q, in_q, out_r, in_r, top_out_q, top_in_q, top_out_r,
    top_in_r, run, st_out, st_in, ls_out, ls_in, kl_out, loss_out,
    g_recv, g_send, src_send, w_sem, d_send, d_recv, y_send, y_recv, st_send, st_recv, ls_send, ls_recv, out_sem,
):
    tok, wide = th_ref.shape
    narrow = sh_ref.shape[1]
    quarter, half = tok // 4, tok // 2
    n_y = n_dp // 2
    per = n_vocab // n_dp
    n = tw_ref.shape[1] // cols
    phases = [(k, early) for k in range(1, n_y) for early in (True, False)] + [(0, False)]
    total = len(phases) * n
    n_far = 8 * (n_y - 1)
    n_slots = n_far + 4

    d, v = lax.axis_index("dp"), lax.axis_index("vocab")
    y, core = d // 2, lax.rem(d, 2)
    row, col = v // per, lax.rem(v, per)

    def remote(src, dst, send, recv, dp, vocab):
        return pltpu.make_async_remote_copy(
            src_ref=src, dst_ref=dst, send_sem=send, recv_sem=recv,
            device_id={"dp": dp, "vocab": vocab}, device_id_type=MESH,
        )

    def weight_copies(g):
        at = pl.ds(pl.multiple_of(lax.rem(g, n) * cols, LANES), cols)
        slot = lax.rem(g, SLOTS)
        return (
            pltpu.make_async_copy(tw_ref.at[:, at], wt.at[slot], w_sem.at[slot, 0]),
            pltpu.make_async_copy(sw_ref.at[:, at], ws.at[slot], w_sem.at[slot, 1]),
        )

    def weights_start(g):
        for copy in weight_copies(g):
            copy.start()

    for g in range(SLOTS - 1):
        weights_start(jnp.int32(g))

    barrier = pltpu.get_barrier_semaphore()
    for o in range(1, n_dp):
        pl.semaphore_signal(barrier, inc=1, device_id={"dp": lax.rem(d + o, n_dp), "vocab": v}, device_id_type=MESH)
    for o in range(1, n_vocab):
        pl.semaphore_signal(barrier, inc=1, device_id={"dp": d, "vocab": lax.rem(v + o, n_vocab)}, device_id_type=MESH)
    with jax.named_scope("barrier"):
        pl.semaphore_wait(barrier, n_dp + n_vocab - 2)

    heads = ((th_ref, hid_t, wide), (sh_ref, hid_s, narrow))

    def place(s):
        if s >= n_far:
            rel, h = divmod(s - n_far, 2)
            return (n_y - 1) * 2 * tok + rel * tok + h * half, half, h * half
        k, at = divmod(s, 8)
        j, rel = divmod(at, 2)
        inside = rel * quarter if j == 0 else 2 * quarter + (3 * rel + j - 1) * quarter
        return k * 2 * tok + inside, quarter, j * quarter

    def slots_of(k, rel):
        if k:
            return [(k - 1) * 8 + j * 2 + rel for j in range(4)]
        return [n_far + rel * 2 + h for h in range(2)]

    def region(hid, s, q, width):
        first, size, _ = place(s)
        return hid.at[pl.ds(first, size), pl.ds(pl.multiple_of(q * width, LANES), width)]

    y_to, core_to = row // 2, lax.rem(row, 2)
    k_of, rel_of = lax.rem(y - y_to + n_y, n_y), lax.rem(core + core_to, 2)

    def source_copies(k, rel):
        out = []
        for i, s in enumerate(slots_of(k, rel)):
            _, size, first = place(s)
            for e, (src, hid, width) in enumerate(heads):
                piece, at, recv = src.at[pl.ds(first, size), :], region(hid, s, col, width), g_recv.at[col, s, e]
                if k or rel:
                    out.append(remote(piece, at, src_send.at[i, e], recv, row, v))
                else:
                    out.append(pltpu.make_async_copy(piece, at, recv))
        return out

    def each_source(act, local=True):
        for k in range(n_y):
            for rel in range(0 if k or local else 1, 2):

                @pl.when((k_of == k) & (rel_of == rel))
                def _(k=k, rel=rel):
                    for copy in source_copies(k, rel):
                        act(copy)

    each_source(lambda copy: copy.start())

    def arrived(s, q):
        for e, (_, hid, width) in enumerate(heads):
            at = region(hid, s, q, width)
            pltpu.make_async_copy(at, at, g_recv.at[q, s, e]).wait()

    up, down = (row >= d) & (row + 1 < n_dp), (row <= d) & (row > 0)

    def forwards(s, e):
        _, hid, width = heads[e]
        at = region(hid, s, col, width)
        recv = g_recv.at[col, s, e]
        peers = [
            remote(at, at, g_send.at[s, e, 1 + o], recv, d, row * per + lax.rem(col + o, per)) for o in range(1, per)
        ]
        return (
            remote(at, at, g_send.at[s, e, 0], recv, d, lax.rem(v + per, n_vocab)),
            remote(at, at, g_send.at[s, e, 1], recv, d, lax.rem(v + n_vocab - per, n_vocab)),
            peers,
        )

    def relay_wait(s, e):
        _, hid, width = heads[e]
        at = region(hid, s, col, width)
        pltpu.make_async_copy(at, at, g_recv.at[col, s, e]).wait()

    def relay_send(s, e):
        above, below, peers = forwards(s, e)

        @pl.when(up)
        def _():
            above.start()

        @pl.when(down)
        def _():
            below.start()

        for copy in peers:
            copy.start()

    def relay(s):
        for e in range(2):
            relay_wait(s, e)
            relay_send(s, e)

    def peers_arrived(s):
        for o in range(1, per):
            arrived(s, lax.rem(col + o, per))

    away = jnp.abs(row - d)
    moved, moved_far = jnp.minimum(away, 1), jnp.minimum(away // 2, 1)
    longest = 1 - jnp.minimum(jnp.minimum(d, n_dp - 1 - d), 1)

    def slots_in(f):
        k, early = phases[f]
        if k == 0:
            return range(n_far, n_slots)
        first = (k - 1) * 8
        return range(first, first + 2) if early else range(first + 2, first + 8)

    def relay_step(s):
        f = next(f for f in range(len(phases)) if s in slots_in(f))
        if s >= n_far:
            usual = LATE + SPACE * (s - n_far) + HOP * away
        else:
            j = (s % 8) // 2
            first = moved_far * (4 * j - 3 + 3 * (away - 2))
            other = moved * (4 * j + 2 * (away - 1)) + (1 - moved) * (-1 if s < 8 else 1)
            usual = (s // 8) * 2 * n + (longest * first + (1 - longest) * other if j else 0)
        return jnp.minimum(usual, max(f * n - 1, 0))

    def rows_of(f):
        k, early = phases[f]
        if k == 0:
            return (n_y - 1) * 2 * tok, tok
        return (k - 1) * 2 * tok + (0 if early else 2 * quarter), quarter if early else 3 * quarter

    def matmul(g, f):
        first, size = rows_of(f)
        slot, at = lax.rem(g, SLOTS), lax.rem(g, 2)
        x_t, x_s = hid_t[first : first + 2 * size, :], hid_s[first : first + 2 * size, :]
        part[at, 0, pl.ds(0, 2 * size), :] = jnp.dot(x_t, wt[slot], preferred_element_type=jnp.float32)
        part[at, 1, pl.ds(0, 2 * size), :] = jnp.dot(x_s, ws[slot], preferred_element_type=jnp.float32)

    partner = d + 1 - 2 * core

    def pair_buffer(f, i):
        k, early = phases[f]
        if k == 0:
            return pair_b.at[i]
        return (pair_q if early else pair_r).at[(k - 1) * n + i]

    def pair_copy(f, i):
        g = f * n + i
        at, size = lax.rem(g, 2), rows_of(f)[1]
        return remote(
            part.at[at, :, pl.ds(size, size), :], pair_buffer(f, i), d_send.at[at], d_recv.at[g], partner, v
        )

    def code_copies(f, i):
        k, early = phases[f]
        at, g = (k - 1) * n + i, f * n + i
        to = lax.rem(y + k, n_y) * 2 + core
        code_out, code_in = (out_q, in_q) if early else (out_r, in_r)
        top_out, top_in = (top_out_q, top_in_q) if early else (top_out_r, top_in_r)
        return (
            remote(code_out.at[at], code_in.at[at], y_send.at[g, 0], y_recv.at[g, 0], to, v),
            remote(top_out.at[at], top_in.at[at], y_send.at[g, 1], y_recv.at[g, 1], to, v),
        )

    def code_start(f, i):
        if phases[f][0]:
            for copy in code_copies(f, i):
                copy.start()

    def finish_far(f, i):
        k, early = phases[f]
        at, size = (k - 1) * n + i, rows_of(f)[1]
        slot = lax.rem(f * n + i, 2)
        pair_copy(f, i).wait()
        code_out, top_out, pair = (out_q, top_out_q, pair_q) if early else (out_r, top_out_r, pair_r)
        tops = []
        for e in range(2):
            code, top = encode(part[slot, e, pl.ds(0, size), :] + pair[at, e])
            code_out[at, e] = code
            tops.append(jnp.broadcast_to(top, (size, LANES)))
        spare = top_out.shape[2] - 2 * size
        tops = jnp.concatenate(tops + [jnp.zeros((spare, LANES), jnp.float32)], axis=0)
        top_out[at] = tops.T[:8]

    def absorb(first, size, t, s):
        rows = pl.ds(first, size)
        ts = [t[:, b * LANES : (b + 1) * LANES] for b in range(cols // LANES)]
        ss = [s[:, b * LANES : (b + 1) * LANES] for b in range(cols // LANES)]
        t_old, s_old = run[0, rows, :], run[1, rows, :]
        t_top = functools.reduce(jnp.maximum, ts, t_old)
        s_top = functools.reduce(jnp.maximum, ss, s_old)
        t_fix = jnp.exp(t_old - t_top)
        t_sum, w_sum = run[2, rows, :] * t_fix, run[3, rows, :] * t_fix
        s_sum = run[4, rows, :] * jnp.exp(s_old - s_top)
        for tb, sb in zip(ts, ss):
            e = jnp.exp(tb - t_top)
            t_sum = t_sum + e
            w_sum = w_sum + e * (tb - sb)
            s_sum = s_sum + jnp.exp(sb - s_top)
        run[0, rows, :], run[1, rows, :] = t_top, s_top
        run[2, rows, :], run[3, rows, :], run[4, rows, :] = t_sum, w_sum, s_sum

    def finish_near(f, i):
        slot = lax.rem(f * n + i, 2)
        pair_copy(f, i).wait()
        for o in range(len(phases) - 1):
            for copy in code_copies(o, i):
                with jax.named_scope("ywait"):
                    copy.wait_recv()
        for early in (True, False):
            first, size = (0, quarter) if early else (quarter, 3 * quarter)
            code_in, top_in = (in_q, top_in_q) if early else (in_r, top_in_r)
            t, s = (
                part[slot, e, pl.ds(first, size), :] + pair_b[i, e, pl.ds(first, size), :] for e in range(2)
            )
            for k in range(1, n_y):
                at = (k - 1) * n + i
                scale = (jnp.broadcast_to(top_in[at][:1], (LANES, top_in.shape[2])).T) * (1.0 / SPAN)
                blocks = cols // LANES
                t = t + decode(code_in[at, 0], jnp.concatenate([scale[:size]] * blocks, axis=1))
                s = s + decode(code_in[at, 1], jnp.concatenate([scale[size : 2 * size]] * blocks, axis=1))
            absorb(first, size, t, s)

    def finish(f, i):
        if phases[f][0]:
            finish_far(f, i)
        else:
            finish_near(f, i)

    run[pl.ds(0, 2)] = jnp.full((2, tok, LANES), -jnp.inf, jnp.float32)
    run[pl.ds(2, 3)] = jnp.zeros((3, tok, LANES), jnp.float32)

    for f in range(len(phases)):

        def step(i, _, f=f):
            g = f * n + i

            @pl.when(i >= 1)
            def _():
                pair_copy(f, i - 1).start()

            @pl.when(i >= 2)
            def _():
                code_start(f, i - 2)

            if f:

                @pl.when(i == 0)
                def _():
                    pair_copy(f - 1, jnp.int32(n - 1)).start()
                    code_start(f - 1, jnp.int32(n - 2))

                @pl.when(i == 1)
                def _():
                    code_start(f - 1, jnp.int32(n - 1))

            if f == 0:
                @pl.when((i == 1) & (away == 0) & (longest == 0))
                def _():
                    with jax.named_scope("relay"):
                        for act in (relay_wait, relay_send):
                            for s in range(2, 8):
                                for e in range(2):
                                    act(s, e)

            if f < len(phases) - 1:
                for s in range(slots_in(f).start, n_slots):

                    @pl.when(g == relay_step(s))
                    def _(s=s):
                        with jax.named_scope("relay"):
                            relay(s)

            @pl.when(i == 0)
            def _():
                with jax.named_scope("peers"):
                    for s in slots_in(f):
                        peers_arrived(s)

            with jax.named_scope("wwait"):
                for copy in weight_copies(g):
                    copy.wait()

            @pl.when(g + SLOTS - 1 < total)
            def _():
                weights_start(g + SLOTS - 1)

            with jax.named_scope("mm"):
                matmul(g, f)

            @pl.when(i >= 1)
            def _():
                with jax.named_scope("finish"):
                    finish(f, i - 1)

            if f:

                @pl.when(i == 0)
                def _():
                    with jax.named_scope("finish"):
                        finish(f - 1, jnp.int32(n - 1))

            return 0

        lax.fori_loop(0, n, step, 0)

    last = len(phases) - 1
    pair_copy(last, jnp.int32(n - 1)).start()
    finish(last, jnp.int32(n - 1))

    t_lane, s_lane = run[0], run[1]
    t_top = jnp.max(t_lane, axis=1, keepdims=True)
    s_top = jnp.max(s_lane, axis=1, keepdims=True)
    t_fix = jnp.exp(t_lane - t_top)
    t_sum = jnp.sum(run[2] * t_fix, axis=1, keepdims=True)
    w_sum = jnp.sum(run[3] * t_fix, axis=1, keepdims=True)
    s_sum = jnp.sum(run[4] * jnp.exp(s_lane - s_top), axis=1, keepdims=True)
    lane = lax.broadcasted_iota(jnp.int32, (tok, LANES), 1)
    table = jnp.zeros((tok, LANES), jnp.float32)
    for i, stat in enumerate((t_top, s_top, t_sum, w_sum, s_sum)):
        table = jnp.where(lane == i, stat, table)
    table = table.T[:8]
    st_out[...] = table
    st_in[v] = table

    each_source(lambda copy: copy.wait_send(), local=False)

    for f in range(last):

        def drain_codes(i, _, f=f):
            for copy in code_copies(f, i):
                copy.wait_send()
            return 0

        lax.fori_loop(0, n, drain_codes, 0)

    for s in range(n_slots):
        for e in range(2):
            above, below, peers = forwards(s, e)

            @pl.when(up)
            def _():
                above.wait_send()

            @pl.when(down)
            def _():
                below.wait_send()

            for copy in peers:
                copy.wait_send()

    def stat_copy(to, holder):
        return remote(st_out, st_in.at[holder], st_send.at[to], st_recv.at[holder], d, to)

    others = [lax.rem(v + o, n_vocab) for o in range(1, n_vocab)]
    for o in others:
        stat_copy(o, v).start()
    with jax.named_scope("statwait"):
        for o in others:
            stat_copy(v, o).wait_recv()

    def field(holder, i):
        return st_in[holder, pl.ds(i, 1), :]

    t_max = functools.reduce(jnp.maximum, [field(q, 0) for q in range(n_vocab)])
    s_max = functools.reduce(jnp.maximum, [field(q, 1) for q in range(n_vocab)])
    t_total = weighted = s_total = jnp.zeros((1, tok), jnp.float32)
    for q in range(n_vocab):
        scale = jnp.exp(field(q, 0) - t_max)
        t_total = t_total + scale * field(q, 2)
        weighted = weighted + scale * field(q, 3)
        s_total = s_total + jnp.exp(field(q, 1) - s_max) * field(q, 4)
    kl = weighted / t_total - (t_max + jnp.log(t_total)) + (s_max + jnp.log(s_total))
    kl_out[...] = kl
    mine = jnp.broadcast_to(jnp.sum(kl, axis=1, keepdims=True), (8, LANES))
    ls_out[...] = mine
    ls_in[d] = mine
    for o in others:
        stat_copy(o, v).wait_send()

    def loss_copy(to, holder):
        return remote(ls_out, ls_in.at[holder], ls_send.at[to], ls_recv.at[holder], to, v)

    others = [lax.rem(d + o, n_dp) for o in range(1, n_dp)]
    for o in others:
        loss_copy(o, d).start()
    kl_write = pltpu.make_async_copy(kl_out, kl_ref, out_sem.at[0])
    kl_write.start()
    with jax.named_scope("losswait"):
        for o in others:
            loss_copy(d, o).wait_recv()
    loss = functools.reduce(jnp.add, [ls_in[q] for q in range(n_dp)]) / (tok * n_dp)
    loss_out[...] = loss[:1, :1]
    for o in others:
        loss_copy(o, d).wait_send()
    loss_write = pltpu.make_async_copy(loss_out, loss_ref, out_sem.at[1])
    loss_write.start()
    loss_write.wait()
    kl_write.wait()


def shards(teacher_hidden, student_hidden, teacher_weight, student_weight):
    n_dp, n_vocab = lax.axis_size("dp"), lax.axis_size("vocab")
    tok, wide = teacher_hidden.shape
    narrow = student_hidden.shape[1]
    deep, local_cols = teacher_weight.shape
    shallow = student_weight.shape[0]
    cols = min(512, local_cols)
    n, n_y, per = local_cols // cols, n_dp // 2, n_vocab // n_dp
    few, many = tok // 4, 3 * tok // 4
    far = (n_y - 1) * n
    slots = 8 * (n_y - 1) + 4
    steps = 2 * far + n
    top_few, top_many = (-(-2 * rows // LANES) * LANES for rows in (few, many))
    bf16, f32, dma = jnp.bfloat16, jnp.float32, pltpu.SemaphoreType.DMA
    hbm = pl.BlockSpec(memory_space=pl.ANY)
    kl, loss = pl.pallas_call(
        functools.partial(kernel, n_dp, n_vocab, cols),
        out_shape=(jax.ShapeDtypeStruct((1, tok), f32), jax.ShapeDtypeStruct((1, 1), f32)),
        in_specs=[hbm] * 4,
        out_specs=(hbm, hbm),
        scratch_shapes=[
            pltpu.VMEM((n_dp * tok, deep), bf16),
            pltpu.VMEM((n_dp * tok, shallow), bf16),
            pltpu.VMEM((SLOTS, deep, cols), bf16),
            pltpu.VMEM((SLOTS, shallow, cols), bf16),
            pltpu.VMEM((2, 2, 2 * tok, cols), f32),
            pltpu.VMEM((far, 2, few, cols), f32),
            pltpu.VMEM((far, 2, many, cols), f32),
            pltpu.VMEM((n, 2, tok, cols), f32),
            pltpu.VMEM((far, 2, few, cols), bf16),
            pltpu.VMEM((far, 2, few, cols), bf16),
            pltpu.VMEM((far, 2, many, cols), bf16),
            pltpu.VMEM((far, 2, many, cols), bf16),
            pltpu.VMEM((far, 8, top_few), f32),
            pltpu.VMEM((far, 8, top_few), f32),
            pltpu.VMEM((far, 8, top_many), f32),
            pltpu.VMEM((far, 8, top_many), f32),
            pltpu.VMEM((5, tok, LANES), f32),
            pltpu.VMEM((8, tok), f32),
            pltpu.VMEM((n_vocab, 8, tok), f32),
            pltpu.VMEM((8, LANES), f32),
            pltpu.VMEM((n_dp, 8, LANES), f32),
            pltpu.VMEM((1, tok), f32),
            pltpu.VMEM((1, 1), f32),
            dma((per, slots, 2)),
            dma((slots, 2, per + 1)),
            dma((4, 2)),
            dma((SLOTS, 2)),
            dma((2,)),
            dma((steps,)),
            dma((2 * far, 2)),
            dma((2 * far, 2)),
            dma((n_vocab,)),
            dma((n_vocab,)),
            dma((n_dp,)),
            dma((n_dp,)),
            dma((2,)),
        ],
        compiler_params=pltpu.CompilerParams(
            collective_id=0, has_side_effects=True, vmem_limit_bytes=64 * 1024 * 1024 - 65536
        ),
    )(teacher_hidden, student_hidden, teacher_weight, student_weight)
    return kl.reshape(tok), loss.reshape(())


def solution(mesh):
    in_specs = (P("dp", "vocab"), P("dp", "vocab"), P("dp", "vocab"), P("dp", "vocab"))
    out_specs = (P("dp"), P())
    return jax.shard_map(shards, mesh=mesh, in_specs=in_specs, out_specs=out_specs, check_vma=False)
```

```python
import functools

import jax
import jax.numpy as jnp
from jax import lax
from jax.experimental import pallas as pl
from jax.experimental.pallas import tpu as pltpu
from jax.sharding import PartitionSpec as P

MESH = pl.DeviceIdType.MESH
SPAN = 240.0
LANES = 128
SLOTS = 3
HOP = 2
SPACE = 4
LATE = 14


def encode(block):
    mag = jnp.abs(block)
    top = jnp.max(mag, axis=1, keepdims=True)
    step = jnp.where(top > 0, SPAN / jnp.where(top > 0, top, 1.0), 0.0)
    power = jnp.exp2(mag * step - 0.5 * SPAN)
    return jnp.where(block < 0, -power, power).astype(jnp.bfloat16), top


def decode(code, scale):
    value = code.astype(jnp.float32)
    mag = (jnp.log2(jnp.abs(value)) + 0.5 * SPAN) * scale
    return jnp.where(value < 0, -mag, mag)


def kernel(
    n_dp, n_vocab, cols,
    th_ref, sh_ref, tw_ref, sw_ref, kl_ref, loss_ref,
    hid_t, hid_s, wt, ws, part, pair_q, pair_r, pair_b, out_q, in_q, out_r, in_r, top_out_q, top_in_q, top_out_r,
    top_in_r, run, st_out, st_in, ls_out, ls_in, kl_out, loss_out,
    g_recv, g_send, src_send, w_sem, d_send, d_recv, y_send, y_recv, st_send, st_recv, ls_send, ls_recv, out_sem,
):
    tok, wide = th_ref.shape
    narrow = sh_ref.shape[1]
    quarter, half = tok // 4, tok // 2
    n_y = n_dp // 2
    per = n_vocab // n_dp
    n = tw_ref.shape[1] // cols
    phases = [(k, early) for k in range(1, n_y) for early in (True, False)] + [(0, False)]
    total = len(phases) * n
    n_far = 8 * (n_y - 1)
    n_slots = n_far + 4

    d, v = lax.axis_index("dp"), lax.axis_index("vocab")
    y, core = d // 2, lax.rem(d, 2)
    row, col = v // per, lax.rem(v, per)

    def remote(src, dst, send, recv, dp, vocab):
        return pltpu.make_async_remote_copy(
            src_ref=src, dst_ref=dst, send_sem=send, recv_sem=recv,
            device_id={"dp": dp, "vocab": vocab}, device_id_type=MESH,
        )

    def weight_copies(g):
        at = pl.ds(pl.multiple_of(lax.rem(g, n) * cols, LANES), cols)
        slot = lax.rem(g, SLOTS)
        return (
            pltpu.make_async_copy(tw_ref.at[:, at], wt.at[slot], w_sem.at[slot, 0]),
            pltpu.make_async_copy(sw_ref.at[:, at], ws.at[slot], w_sem.at[slot, 1]),
        )

    def weights_start(g):
        for copy in weight_copies(g):
            copy.start()

    for g in range(SLOTS - 1):
        weights_start(jnp.int32(g))

    barrier = pltpu.get_barrier_semaphore()
    for o in range(1, n_dp):
        pl.semaphore_signal(barrier, inc=1, device_id={"dp": lax.rem(d + o, n_dp), "vocab": v}, device_id_type=MESH)
    for o in range(1, n_vocab):
        pl.semaphore_signal(barrier, inc=1, device_id={"dp": d, "vocab": lax.rem(v + o, n_vocab)}, device_id_type=MESH)
    with jax.named_scope("barrier"):
        pl.semaphore_wait(barrier, n_dp + n_vocab - 2)

    heads = ((th_ref, hid_t, wide), (sh_ref, hid_s, narrow))

    def place(s):
        if s >= n_far:
            rel, h = divmod(s - n_far, 2)
            return (n_y - 1) * 2 * tok + rel * tok + h * half, half, h * half
        k, at = divmod(s, 8)
        j, rel = divmod(at, 2)
        inside = rel * quarter if j == 0 else 2 * quarter + (3 * rel + j - 1) * quarter
        return k * 2 * tok + inside, quarter, j * quarter

    def slots_of(k, rel):
        if k:
            return [(k - 1) * 8 + j * 2 + rel for j in range(4)]
        return [n_far + rel * 2 + h for h in range(2)]

    def region(hid, s, q, width):
        first, size, _ = place(s)
        return hid.at[pl.ds(first, size), pl.ds(pl.multiple_of(q * width, LANES), width)]

    y_to, core_to = row // 2, lax.rem(row, 2)
    k_of, rel_of = lax.rem(y - y_to + n_y, n_y), lax.rem(core + core_to, 2)

    def source_copies(k, rel):
        out = []
        for s in slots_of(k, rel):
            _, size, first = place(s)
            for e, (src, hid, width) in enumerate(heads):
                piece, at, recv = src.at[pl.ds(first, size), :], region(hid, s, col, width), g_recv.at[col, s, e]
                if k or rel:
                    out.append(remote(piece, at, src_send.at[e], recv, row, v))
                else:
                    out.append(pltpu.make_async_copy(piece, at, recv))
        return out

    for k in range(n_y):
        for rel in range(2):

            @pl.when((k_of == k) & (rel_of == rel))
            def _(k=k, rel=rel):
                for copy in source_copies(k, rel):
                    copy.start()

    def arrived(s, q):
        for e, (_, hid, width) in enumerate(heads):
            at = region(hid, s, q, width)
            pltpu.make_async_copy(at, at, g_recv.at[q, s, e]).wait()

    up, down = (row >= d) & (row + 1 < n_dp), (row <= d) & (row > 0)

    def forwards(s, e):
        _, hid, width = heads[e]
        at = region(hid, s, col, width)
        recv = g_recv.at[col, s, e]
        peers = [
            remote(at, at, g_send.at[e, 1 + o], recv, d, row * per + lax.rem(col + o, per)) for o in range(1, per)
        ]
        return (
            remote(at, at, g_send.at[e, 0], recv, d, lax.rem(v + per, n_vocab)),
            remote(at, at, g_send.at[e, 1], recv, d, lax.rem(v + n_vocab - per, n_vocab)),
            peers,
        )

    def relay_wait(s, e):
        _, hid, width = heads[e]
        at = region(hid, s, col, width)
        pltpu.make_async_copy(at, at, g_recv.at[col, s, e]).wait()

    def relay_send(s, e):
        above, below, peers = forwards(s, e)

        @pl.when(up)
        def _():
            above.start()

        @pl.when(down)
        def _():
            below.start()

        for copy in peers:
            copy.start()

    def relay(s):
        for e in range(2):
            relay_wait(s, e)
            relay_send(s, e)

    def peers_arrived(s):
        for o in range(1, per):
            arrived(s, lax.rem(col + o, per))

    away = jnp.abs(row - d)
    moved, moved_far = jnp.minimum(away, 1), jnp.minimum(away // 2, 1)
    longest = 1 - jnp.minimum(jnp.minimum(d, n_dp - 1 - d), 1)

    def slots_in(f):
        k, early = phases[f]
        if k == 0:
            return range(n_far, n_slots)
        first = (k - 1) * 8
        return range(first, first + 2) if early else range(first + 2, first + 8)

    def relay_step(s):
        f = next(f for f in range(len(phases)) if s in slots_in(f))
        if s >= n_far:
            usual = LATE + SPACE * (s - n_far) + HOP * away - 3 * (1 - longest) * (1 - moved)
        else:
            j = (s % 8) // 2
            first = moved_far * (4 * j - 3 + away - 2)
            other = moved * (4 * j - 1 + 2 * (away - 1)) + (1 - moved) * (-1 if s < 8 else 1)
            usual = (s // 8) * 2 * n + (longest * first + (1 - longest) * other if j else 0)
        return jnp.minimum(usual, max(f * n - 1, 0))

    def rows_of(f):
        k, early = phases[f]
        if k == 0:
            return (n_y - 1) * 2 * tok, tok
        return (k - 1) * 2 * tok + (0 if early else 2 * quarter), quarter if early else 3 * quarter

    def matmul(g, f):
        first, size = rows_of(f)
        slot, at = lax.rem(g, SLOTS), lax.rem(g, 2)
        x_t, x_s = hid_t[first : first + 2 * size, :], hid_s[first : first + 2 * size, :]
        part[at, 0, pl.ds(0, 2 * size), :] = jnp.dot(x_t, wt[slot], preferred_element_type=jnp.float32)
        part[at, 1, pl.ds(0, 2 * size), :] = jnp.dot(x_s, ws[slot], preferred_element_type=jnp.float32)

    partner = d + 1 - 2 * core

    def pair_buffer(f, i):
        k, early = phases[f]
        if k == 0:
            return pair_b.at[i]
        return (pair_q if early else pair_r).at[(k - 1) * n + i]

    def pair_copy(f, i):
        g = f * n + i
        at, size = lax.rem(g, 2), rows_of(f)[1]
        return remote(
            part.at[at, :, pl.ds(size, size), :], pair_buffer(f, i), d_send.at[at], d_recv.at[g], partner, v
        )

    def code_copies(f, i):
        k, early = phases[f]
        at, g = (k - 1) * n + i, f * n + i
        to = lax.rem(y + k, n_y) * 2 + core
        early = int(early)
        code_out, code_in = (out_q, in_q) if early else (out_r, in_r)
        top_out, top_in = (top_out_q, top_in_q) if early else (top_out_r, top_in_r)
        return (
            remote(code_out.at[at], code_in.at[at], y_send.at[early, 0], y_recv.at[g, 0], to, v),
            remote(top_out.at[at], top_in.at[at], y_send.at[early, 1], y_recv.at[g, 1], to, v),
        )

    def code_start(f, i):
        if phases[f][0]:
            for copy in code_copies(f, i):
                copy.start()

    def finish_far(f, i):
        k, early = phases[f]
        at, size = (k - 1) * n + i, rows_of(f)[1]
        slot = lax.rem(f * n + i, 2)
        pair_copy(f, i).wait()
        code_out, top_out, pair = (out_q, top_out_q, pair_q) if early else (out_r, top_out_r, pair_r)
        tops = []
        for e in range(2):
            code, top = encode(part[slot, e, pl.ds(0, size), :] + pair[at, e])
            code_out[at, e] = code
            tops.append(jnp.broadcast_to(top, (size, LANES)))
        spare = top_out.shape[2] - 2 * size
        tops = jnp.concatenate(tops + [jnp.zeros((spare, LANES), jnp.float32)], axis=0)
        top_out[at] = tops.T[:8]

    def absorb(first, size, t, s):
        rows = pl.ds(first, size)
        ts = [t[:, b * LANES : (b + 1) * LANES] for b in range(cols // LANES)]
        ss = [s[:, b * LANES : (b + 1) * LANES] for b in range(cols // LANES)]
        t_old, s_old = run[0, rows, :], run[1, rows, :]
        t_top = functools.reduce(jnp.maximum, ts, t_old)
        s_top = functools.reduce(jnp.maximum, ss, s_old)
        t_fix = jnp.exp(t_old - t_top)
        t_sum, w_sum = run[2, rows, :] * t_fix, run[3, rows, :] * t_fix
        s_sum = run[4, rows, :] * jnp.exp(s_old - s_top)
        for tb, sb in zip(ts, ss):
            e = jnp.exp(tb - t_top)
            t_sum = t_sum + e
            w_sum = w_sum + e * (tb - sb)
            s_sum = s_sum + jnp.exp(sb - s_top)
        run[0, rows, :], run[1, rows, :] = t_top, s_top
        run[2, rows, :], run[3, rows, :], run[4, rows, :] = t_sum, w_sum, s_sum

    def finish_near(f, i):
        slot = lax.rem(f * n + i, 2)
        pair_copy(f, i).wait()
        for o in range(len(phases) - 1):
            for copy in code_copies(o, i):
                with jax.named_scope("ywait"):
                    copy.wait_recv()
        for early in (True, False):
            first, size = (0, quarter) if early else (quarter, 3 * quarter)
            code_in, top_in = (in_q, top_in_q) if early else (in_r, top_in_r)
            t, s = (
                part[slot, e, pl.ds(first, size), :] + pair_b[i, e, pl.ds(first, size), :] for e in range(2)
            )
            for k in range(1, n_y):
                at = (k - 1) * n + i
                scale = (jnp.broadcast_to(top_in[at][:1], (LANES, top_in.shape[2])).T) * (1.0 / SPAN)
                blocks = cols // LANES
                t = t + decode(code_in[at, 0], jnp.concatenate([scale[:size]] * blocks, axis=1))
                s = s + decode(code_in[at, 1], jnp.concatenate([scale[size : 2 * size]] * blocks, axis=1))
            absorb(first, size, t, s)

    def finish(f, i):
        if phases[f][0]:
            finish_far(f, i)
        else:
            finish_near(f, i)

    run[pl.ds(0, 2)] = jnp.full((2, tok, LANES), -jnp.inf, jnp.float32)
    run[pl.ds(2, 3)] = jnp.zeros((3, tok, LANES), jnp.float32)

    for f in range(len(phases)):

        def step(i, _, f=f):
            g = f * n + i

            @pl.when(i >= 1)
            def _():
                pair_copy(f, i - 1).start()

            @pl.when(i >= 2)
            def _():
                code_start(f, i - 2)

            if f:

                @pl.when(i == 0)
                def _():
                    pair_copy(f - 1, jnp.int32(n - 1)).start()
                    code_start(f - 1, jnp.int32(n - 2))

                @pl.when(i == 1)
                def _():
                    code_start(f - 1, jnp.int32(n - 1))

            if f == 0:
                @pl.when((i == 1) & (away == 0) & (longest == 0))
                def _():
                    with jax.named_scope("relay"):
                        for act in (relay_wait, relay_send):
                            for s in range(2, 8):
                                for e in range(2):
                                    act(s, e)

            if f < len(phases) - 1:
                for s in range(slots_in(f).start, n_slots):

                    @pl.when(g == relay_step(s))
                    def _(s=s):
                        with jax.named_scope("relay"):
                            relay(s)

            @pl.when(i == 0)
            def _():
                with jax.named_scope("peers"):
                    for s in slots_in(f):
                        peers_arrived(s)

            with jax.named_scope("wwait"):
                for copy in weight_copies(g):
                    copy.wait()

            @pl.when(g + SLOTS - 1 < total)
            def _():
                weights_start(g + SLOTS - 1)

            with jax.named_scope("mm"):
                matmul(g, f)

            @pl.when(i >= 1)
            def _():
                with jax.named_scope("finish"):
                    finish(f, i - 1)

            if f:

                @pl.when(i == 0)
                def _():
                    with jax.named_scope("finish"):
                        finish(f - 1, jnp.int32(n - 1))

            return 0

        lax.fori_loop(0, n, step, 0)

    last = len(phases) - 1
    pair_copy(last, jnp.int32(n - 1)).start()
    finish(last, jnp.int32(n - 1))

    t_lane, s_lane = run[0], run[1]
    t_top = jnp.max(t_lane, axis=1, keepdims=True)
    s_top = jnp.max(s_lane, axis=1, keepdims=True)
    t_fix = jnp.exp(t_lane - t_top)
    t_sum = jnp.sum(run[2] * t_fix, axis=1, keepdims=True)
    w_sum = jnp.sum(run[3] * t_fix, axis=1, keepdims=True)
    s_sum = jnp.sum(run[4] * jnp.exp(s_lane - s_top), axis=1, keepdims=True)
    lane = lax.broadcasted_iota(jnp.int32, (tok, LANES), 1)
    table = jnp.zeros((tok, LANES), jnp.float32)
    for i, stat in enumerate((t_top, s_top, t_sum, w_sum, s_sum)):
        table = jnp.where(lane == i, stat, table)
    table = table.T[:8]
    st_out[...] = table
    st_in[v] = table

    def sent(ref, sem):
        pltpu.make_async_copy(ref, ref, sem).wait()

    @pl.when(row != d)
    def _():
        for e, (src, _, _) in enumerate(heads):
            sent(src, src_send.at[e])

    if n_y > 1:
        for early, refs in enumerate(((out_r, top_out_r), (out_q, top_out_q))):
            for e, ref in enumerate(refs):
                sent(ref, y_send.at[early, e])

    for e, (_, hid, width) in enumerate(heads):
        passed = hid.at[:, pl.ds(pl.multiple_of(col * width, LANES), width)]

        @pl.when(up)
        def _():
            sent(passed, g_send.at[e, 0])

        @pl.when(down)
        def _():
            sent(passed, g_send.at[e, 1])

        for o in range(1, per):
            sent(passed, g_send.at[e, 1 + o])

    def stat_copy(to, holder):
        return remote(st_out, st_in.at[holder], st_send.at[to], st_recv.at[holder], d, to)

    others = [lax.rem(v + o, n_vocab) for o in range(1, n_vocab)]
    for o in others:
        stat_copy(o, v).start()
    with jax.named_scope("statwait"):
        for o in others:
            stat_copy(v, o).wait_recv()

    def field(holder, i):
        return st_in[holder, pl.ds(i, 1), :]

    t_max = functools.reduce(jnp.maximum, [field(q, 0) for q in range(n_vocab)])
    s_max = functools.reduce(jnp.maximum, [field(q, 1) for q in range(n_vocab)])
    t_total = weighted = s_total = jnp.zeros((1, tok), jnp.float32)
    for q in range(n_vocab):
        scale = jnp.exp(field(q, 0) - t_max)
        t_total = t_total + scale * field(q, 2)
        weighted = weighted + scale * field(q, 3)
        s_total = s_total + jnp.exp(field(q, 1) - s_max) * field(q, 4)
    kl = weighted / t_total - (t_max + jnp.log(t_total)) + (s_max + jnp.log(s_total))
    kl_out[...] = kl
    mine = jnp.broadcast_to(jnp.sum(kl, axis=1, keepdims=True), (8, LANES))
    ls_out[...] = mine
    ls_in[d] = mine
    for o in others:
        stat_copy(o, v).wait_send()

    def loss_copy(to, holder):
        return remote(ls_out, ls_in.at[holder], ls_send.at[to], ls_recv.at[holder], to, v)

    others = [lax.rem(d + o, n_dp) for o in range(1, n_dp)]
    for o in others:
        loss_copy(o, d).start()
    kl_write = pltpu.make_async_copy(kl_out, kl_ref, out_sem.at[0])
    kl_write.start()
    with jax.named_scope("losswait"):
        for o in others:
            loss_copy(d, o).wait_recv()
    loss = functools.reduce(jnp.add, [ls_in[q] for q in range(n_dp)]) / (tok * n_dp)
    loss_out[...] = loss[:1, :1]
    for o in others:
        loss_copy(o, d).wait_send()
    loss_write = pltpu.make_async_copy(loss_out, loss_ref, out_sem.at[1])
    loss_write.start()
    loss_write.wait()
    kl_write.wait()


def shards(teacher_hidden, student_hidden, teacher_weight, student_weight):
    n_dp, n_vocab = lax.axis_size("dp"), lax.axis_size("vocab")
    tok, wide = teacher_hidden.shape
    narrow = student_hidden.shape[1]
    deep, local_cols = teacher_weight.shape
    shallow = student_weight.shape[0]
    cols = min(512, local_cols)
    n, n_y, per = local_cols // cols, n_dp // 2, n_vocab // n_dp
    few, many = tok // 4, 3 * tok // 4
    far = (n_y - 1) * n
    slots = 8 * (n_y - 1) + 4
    steps = 2 * far + n
    top_few, top_many = (-(-2 * rows // LANES) * LANES for rows in (few, many))
    bf16, f32, dma = jnp.bfloat16, jnp.float32, pltpu.SemaphoreType.DMA
    hbm = pl.BlockSpec(memory_space=pl.ANY)
    kl, loss = pl.pallas_call(
        functools.partial(kernel, n_dp, n_vocab, cols),
        out_shape=(jax.ShapeDtypeStruct((1, tok), f32), jax.ShapeDtypeStruct((1, 1), f32)),
        in_specs=[hbm] * 4,
        out_specs=(hbm, hbm),
        scratch_shapes=[
            pltpu.VMEM((n_dp * tok, deep), bf16),
            pltpu.VMEM((n_dp * tok, shallow), bf16),
            pltpu.VMEM((SLOTS, deep, cols), bf16),
            pltpu.VMEM((SLOTS, shallow, cols), bf16),
            pltpu.VMEM((2, 2, 2 * tok, cols), f32),
            pltpu.VMEM((far, 2, few, cols), f32),
            pltpu.VMEM((far, 2, many, cols), f32),
            pltpu.VMEM((n, 2, tok, cols), f32),
            pltpu.VMEM((far, 2, few, cols), bf16),
            pltpu.VMEM((far, 2, few, cols), bf16),
            pltpu.VMEM((far, 2, many, cols), bf16),
            pltpu.VMEM((far, 2, many, cols), bf16),
            pltpu.VMEM((far, 8, top_few), f32),
            pltpu.VMEM((far, 8, top_few), f32),
            pltpu.VMEM((far, 8, top_many), f32),
            pltpu.VMEM((far, 8, top_many), f32),
            pltpu.VMEM((5, tok, LANES), f32),
            pltpu.VMEM((8, tok), f32),
            pltpu.VMEM((n_vocab, 8, tok), f32),
            pltpu.VMEM((8, LANES), f32),
            pltpu.VMEM((n_dp, 8, LANES), f32),
            pltpu.VMEM((1, tok), f32),
            pltpu.VMEM((1, 1), f32),
            dma((per, slots, 2)),
            dma((2, per + 1)),
            dma((2,)),
            dma((SLOTS, 2)),
            dma((2,)),
            dma((steps,)),
            dma((2, 2)),
            dma((2 * far, 2)),
            dma((n_vocab,)),
            dma((n_vocab,)),
            dma((n_dp,)),
            dma((n_dp,)),
            dma((2,)),
        ],
        compiler_params=pltpu.CompilerParams(
            collective_id=0, has_side_effects=True, vmem_limit_bytes=64 * 1024 * 1024 - 65536
        ),
    )(teacher_hidden, student_hidden, teacher_weight, student_weight)
    return kl.reshape(tok), loss.reshape(())


def solution(mesh):
    in_specs = (P("dp", "vocab"), P("dp", "vocab"), P("dp", "vocab"), P("dp", "vocab"))
    out_specs = (P("dp"), P())
    return jax.shard_map(shards, mesh=mesh, in_specs=in_specs, out_specs=out_specs, check_vma=False)
```
